32 devices in a mesh: batch: 8 (over y, x, core), width: 4 (over z).
Axes of the slice: x: 2, y: 2, z: 4, core: 2. Of those that a mesh axis runs over, the one named last changes fastest.
Arguments:
- samples: bfloat16 [2048, 8192], P('batch', 'width'), parts along dimension 0, may hold values from -6 to 6
- rank_down: bfloat16 [8192, 2, 1024], P('width'), may hold values from -0.09375 to 0.09375
- rank_up: bfloat16 [1024, 2, 8192], P(None, None, 'width'), may hold values from -0.1875 to 0.1875
- gate_proj: bfloat16 [8192, 2], P('width'), may hold values from -0.0625 to 0.0625
- expert_bias: float32 [2, 8192], P(None, 'width'), may hold values from -3 to 3
Outputs:
- crossed: bfloat16 [2048, 8192], P('batch', 'width'), parts along dimension 0
The draws below stay inside these ranges and needn't reach their ends.
There are 8 independent parts, one for each index of `batch`. The reference program is written for one: setup_inputs(seed, part) draws one part's arguments, and reference() takes and returns one part's arrays. A program takes and returns all parts, laid end to end along the dimension named above; an argument that names none is the same for every part. Nothing has to cross between parts.
All inputs are finite; a program needn't handle non-finite values.
Results may differ from the reference program's by a relative error of at most 0.0027.
Values may be sent and summed in bfloat16 or wider, within the bound.
No kernel may reach another device: no remote copies, remote signals or barrier semaphores. Data moves between devices by JAX's collectives and lax.ppermute only.
A program may use at most 64 MiB of HBM per device.

```python
import jax
import jax.numpy as jnp

D = 8192
RANK = 1024
EXPERTS = 2
ROWS = 256


def with_spikes(drawn, stream_key, source, target, parts, factor):
    owner, partner = [(jnp.arange(drawn.shape[position]) // (drawn.shape[position] // parts)).reshape([-1 if axis == position else 1 for axis in range(drawn.ndim)]) for position in (source, target)]
    chosen = jax.random.permutation(stream_key, parts)[partner]
    strong = (owner == chosen) | (owner == (partner + parts // 2) % parts)
    return jnp.where(strong, factor * drawn, drawn)


def steps_of(own_key, shape, split, smallest, high):
    def one(axis_at, blocks):
        heights = jax.random.uniform(jax.random.fold_in(jax.random.fold_in(own_key, 6), axis_at), (blocks,), jnp.float32, smallest / len(split), high / len(split))
        return jnp.repeat(jnp.exp(heights), shape[axis_at] // blocks).reshape((-1,) + (1,) * (len(shape) - axis_at - 1))

    loudness = one(*split[0])
    for cut in split[1:]:
        loudness = loudness * one(*cut)
    return loudness


def normal_values(rng, extent, width, most, pieces=(), kind=jnp.bfloat16):
    result = jax.random.normal(rng, extent, jnp.float32) * width
    if len(pieces) > 0:
        result = steps_of(rng, extent, pieces, -0.22, 0.18) * result
    return jnp.clip(result, min=-most, max=most).astype(kind)


def bell_draw_with(own_key, extent, deviation, bound, pieces, heavy, dtype=jnp.bfloat16):
    entries = deviation * jax.random.normal(own_key, extent, jnp.float32)
    if pieces:
        entries = entries * steps_of(own_key, extent, pieces, -0.22, 0.18)
    return jnp.clip(with_spikes(entries, jax.random.fold_in(own_key, 3), *heavy), -bound, bound).astype(dtype)


def setup_inputs(seed: int = 0, part: int = 0) -> dict:
    keys = jax.random.split(jax.random.key(seed), 6)
    part_splits = jax.random.split(jax.random.fold_in(keys[5], part), 6)
    return {
        "samples": normal_values(part_splits[0], (ROWS, D), 1.0, 6.0, ((1, 4),)),
        "rank_down": bell_draw_with(keys[1], (D, EXPERTS, RANK), D ** -0.5, 0.09375, ((0, 4),), (0, 2, 4, 2.0)),
        "rank_up": normal_values(keys[2], (RANK, EXPERTS, D), RANK ** -0.5, 0.1875, ((2, 4),)),
        "gate_proj": normal_values(keys[3], (D, EXPERTS), D ** -0.5, 0.0625, ((0, 4),)),
        "expert_bias": normal_values(keys[4], (EXPERTS, D), 0.5, 3.0, ((1, 4),), jnp.float32),
    }


def reference(samples, rank_down, rank_up, gate_proj, expert_bias):
    inputs = samples.astype(jnp.float32)
    reduced = jnp.einsum("bf,fek->bek", inputs, rank_down.astype(jnp.float32))
    hidden = jnp.tanh(reduced).astype(jnp.bfloat16)
    logits = jnp.dot(samples, gate_proj, preferred_element_type=jnp.float32)
    gating = jax.nn.sigmoid(logits)
    expanded = jnp.einsum("bek,kef->ebf", hidden.astype(jnp.float32), rank_up.astype(jnp.float32))
    blended = jnp.sum(jnp.transpose(gating)[:, :, None] * (expanded + expert_bias[:, None, :]), axis=0)
    return (inputs * blended + inputs).astype(jnp.bfloat16)
```

```python
import jax
import jax.numpy as jnp
from jax import lax
from jax.sharding import PartitionSpec as P


def span(masks):
    out = [0]
    for m in masks:
        out = out + [s ^ m for s in out]
    return out


def swap(value, mask, size):
    return lax.ppermute(value, "width", [(i, i ^ mask) for i in range(size)])


def shards(samples, rank_down, rank_up, gate_proj, expert_bias):
    size = lax.axis_size("width")
    me = lax.axis_index("width")
    experts, rank = rank_down.shape[1:]
    masks = [(2 << i) - 1 for i in range(size.bit_length() - 1)]

    logits = jnp.transpose(jnp.dot(samples, gate_proj, preferred_element_type=jnp.float32))
    for m in masks:
        logits = logits + swap(logits, m, size)
    gating = jax.nn.sigmoid(logits)

    partial = jnp.einsum("bf,fek->ebk", samples, rank_down, preferred_element_type=jnp.float32)
    share = rank // size
    hidden = []
    for e in range(experts):
        order = masks if e % 2 == 0 else masks[::-1]
        held = {
            r: lax.dynamic_slice_in_dim(partial[e], (me ^ r) * share, share, axis=1)
            for r in range(size)
        }
        for i, m in enumerate(order):
            rest = span(order[i + 1 :])
            got = swap(jnp.stack([held[m ^ s] for s in rest]).astype(jnp.bfloat16), m, size)
            held = {s: held[s] + got[j].astype(jnp.float32) for j, s in enumerate(rest)}
        names, have = [0], jnp.tanh(held[0]).astype(jnp.bfloat16)[None]
        for m in order[::-1]:
            names, have = names + [s ^ m for s in names], jnp.concatenate([have, swap(have, m, size)])
        place = jnp.array([names.index(r) for r in range(size)])
        hidden.append(
            jnp.concatenate(
                [lax.dynamic_index_in_dim(have, place[me ^ q], 0, keepdims=False) for q in range(size)], axis=1
            )
        )
    expanded = jnp.einsum("ebk,kef->ebf", jnp.stack(hidden), rank_up, preferred_element_type=jnp.float32)
    blended = jnp.sum(gating[:, :, None] * (expanded + expert_bias[:, None, :]), axis=0)
    inputs = samples.astype(jnp.float32)
    return (inputs * blended + inputs).astype(jnp.bfloat16)


def solution(mesh):
    placed = (
        P("batch", "width"),
        P("width", None, None),
        P(None, None, "width"),
        P("width", None),
        P(None, "width"),
    )
    return jax.shard_map(
        shards, mesh=mesh, in_specs=placed, out_specs=P("batch", "width"), check_vma=False
    )
```

```python
import jax
import jax.numpy as jnp
from jax import lax
from jax.sharding import PartitionSpec as P


def swap(value, bit, size):
    return lax.ppermute(value, "width", [(i, i ^ bit) for i in range(size)])


def side(me, bit):
    return (me & bit) // bit


def half(value, which):
    n = value.shape[1] // 2
    return lax.dynamic_slice_in_dim(value, which * n, n, axis=1)


def hidden_of(partial, order, me, size):
    held = partial
    for bit in order[:-1]:
        mine = side(me, bit)
        got = swap(half(held, 1 - mine).astype(jnp.bfloat16), bit, size)
        held = half(held, mine) + got.astype(jnp.float32)
    for bit in order[-1:]:
        held = held + swap(held.astype(jnp.bfloat16), bit, size).astype(jnp.float32)
    return jnp.tanh(held).astype(jnp.bfloat16)


def shards(samples, rank_down, rank_up, gate_proj, expert_bias):
    size = lax.axis_size("width")
    me = lax.axis_index("width")
    experts = rank_down.shape[1]
    bits = [1 << i for i in range(size.bit_length() - 1)]

    partial = jnp.einsum("bf,fek->ebk", samples, rank_down, preferred_element_type=jnp.float32)
    logits = jnp.transpose(jnp.dot(samples, gate_proj, preferred_element_type=jnp.float32))
    up = jnp.transpose(rank_up, (1, 0, 2))
    hidden = []
    for e in range(experts):
        order = bits if e % 2 == 0 else bits[::-1]
        have = hidden_of(partial[e], order, me, size)
        for bit in order[:-1][::-1]:
            got = swap(have, bit, size)
            first = side(me, bit) == 0
            have = jnp.concatenate([jnp.where(first, have, got), jnp.where(first, got, have)], axis=1)
        hidden.append(have)
    for bit in bits:
        logits = logits + swap(logits, bit, size)
    gating = jax.nn.sigmoid(logits)
    blended = sum(
        gating[e][:, None]
        * (jnp.dot(hidden[e], up[e], preferred_element_type=jnp.float32) + expert_bias[e][None])
        for e in range(experts)
    )
    inputs = samples.astype(jnp.float32)
    return (inputs * blended + inputs).astype(jnp.bfloat16)


def solution(mesh):
    placed = (
        P("batch", "width"),
        P("width", None, None),
        P(None, None, "width"),
        P("width", None),
        P(None, "width"),
    )
    return jax.shard_map(
        shards, mesh=mesh, in_specs=placed, out_specs=P("batch", "width"), check_vma=False
    )
```

```python
import jax
import jax.numpy as jnp
from jax import lax
from jax.sharding import PartitionSpec as P

LANES = 128
BF16 = jnp.bfloat16
F32 = jnp.float32


def swap(value, bit, size):
    return lax.ppermute(value, "width", [(i, i ^ bit) for i in range(size)])


def half(value, which):
    n = value.shape[-1] // 2
    return lax.dynamic_slice_in_dim(value, which * n, n, axis=value.ndim - 1)


def shards(samples, rank_down, rank_up, gate_proj, expert_bias):
    size = lax.axis_size("width")
    me = lax.axis_index("width")
    experts, rank = rank_down.shape[1:]
    bits = [1 << i for i in range(size.bit_length() - 1)]
    orders = [bits, bits[::-1]]
    cut = rank // 2

    held = [
        jnp.einsum("bf,fek->ebk", samples, weights, preferred_element_type=F32)[:, :, -cut:]
        for weights in (rank_down[:, :, :cut], rank_down[:, :, cut - LANES :])
    ]
    logits = jnp.transpose(jnp.dot(samples, gate_proj, preferred_element_type=F32))
    held[0] = lax.optimization_barrier(held[0])
    logits, held[1] = lax.optimization_barrier((logits, held[1]))
    sent = [half(held[s], 1 - me // orders[s][0] % 2).astype(BF16) for s in range(2)]
    arrived = [swap(sent[s], orders[s][0], size) for s in range(2)]
    for bit in bits:
        logits = logits + swap(logits, bit, size)
    gate = jax.nn.sigmoid(logits)

    up = jnp.transpose(rank_up, (1, 0, 2))
    terms = []
    for s, order in enumerate(orders):
        total = half(held[s], me // order[0] % 2) + arrived[s].astype(F32)
        for bit in order[1:-1]:
            mine = me // bit % 2
            part = swap(half(total, 1 - mine).astype(BF16), bit, size)
            total = half(total, mine) + part.astype(F32)
        total = total + swap(total.astype(BF16), order[-1], size).astype(F32)
        have = jnp.tanh(total).astype(BF16)
        for bit in order[:-1][::-1]:
            part = swap(have, bit, size)
            low = me // bit % 2 == 0
            have = jnp.concatenate([jnp.where(low, have, part), jnp.where(low, part, have)], axis=2)
        for e in range(experts):
            terms.append(
                gate[e][:, None]
                * jnp.dot(have[e], up[e, s * cut : (s + 1) * cut], preferred_element_type=F32)
            )
    bias = sum(gate[e][:, None] * expert_bias[e][None] for e in range(experts))
    blended = sum(terms) + bias
    inputs = samples.astype(F32)
    return (inputs * blended + inputs).astype(BF16)


def solution(mesh):
    placed = (
        P("batch", "width"),
        P("width", None, None),
        P(None, None, "width"),
        P("width", None),
        P(None, "width"),
    )
    return jax.shard_map(
        shards, mesh=mesh, in_specs=placed, out_specs=P("batch", "width"), check_vma=False
    )
```

```python
import jax
import jax.numpy as jnp
from jax import lax
from jax.experimental import pallas as pl
from jax.experimental.pallas import tpu as pltpu
from jax.sharding import PartitionSpec as P


LANES = 128
BF16 = jnp.bfloat16
F32 = jnp.float32


def swap(value, bit, size):
    return lax.ppermute(value, "width", [(i, i ^ bit) for i in range(size)])


def turn_kernel(stored_ref, after_ref, out_ref):
    depth, experts, columns = stored_ref.shape
    row = lax.broadcasted_iota(jnp.int32, (experts * depth, experts * depth), 0)
    lane = lax.broadcasted_iota(jnp.int32, (experts * depth, experts * depth), 1)
    ones = (lane == row % depth * experts + row // depth).astype(BF16)
    block = stored_ref[...].reshape(depth * experts, columns)
    turned = jnp.dot(ones, block, preferred_element_type=F32).astype(BF16)
    for e in range(experts):
        out_ref[e] = turned[e * depth : (e + 1) * depth]


def turn(rank_up, start, size, after):
    _, experts, columns = rank_up.shape
    depth = LANES
    return pl.pallas_call(
        turn_kernel,
        grid=(size // depth,),
        in_specs=[
            pl.BlockSpec((depth, experts, columns), lambda i: (start // depth + i, 0, 0)),
            pl.BlockSpec(memory_space=pl.ANY),
        ],
        out_specs=pl.BlockSpec((experts, depth, columns), lambda i: (0, i, 0)),
        out_shape=jax.ShapeDtypeStruct((experts, size, columns), rank_up.dtype),
        compiler_params=pltpu.CompilerParams(vmem_limit_bytes=16 << 20),
        cost_estimate=pl.CostEstimate(
            flops=4 * size * experts * experts * depth * columns,
            bytes_accessed=4 * size * experts * columns,
            transcendentals=0,
        ),
    )(rank_up, after)


def half(value, which):
    n = value.shape[-1] // 2
    return lax.dynamic_slice_in_dim(value, which * n, n, axis=value.ndim - 1)


def layer(samples, rank_down, rank_up, gate_proj, expert_bias):
    size = lax.axis_size("width")
    me = lax.axis_index("width")
    experts, rank = rank_down.shape[1:]
    bits = [1 << i for i in range(size.bit_length() - 1)]
    orders = [bits, bits[::-1]]
    cut = rank // 2

    held = [jnp.einsum("bf,fek->ebk", samples, rank_down[:, :, :cut], preferred_element_type=F32)]
    again, held[0] = lax.optimization_barrier((samples, held[0]))
    wide = jnp.einsum("bf,fek->ebk", again, rank_down[:, :, cut - LANES :], preferred_element_type=F32)
    logits = jnp.transpose(jnp.dot(again, gate_proj, preferred_element_type=F32))
    logits, wide = lax.optimization_barrier((logits, wide[:, :, -cut:]))
    held.append(wide)
    sent = [half(held[s], 1 - me // orders[s][0] % 2).astype(BF16) for s in range(2)]
    arrived = [swap(sent[s], orders[s][0], size) for s in range(2)]
    for bit in bits:
        logits = logits + swap(logits, bit, size)
    gate = jax.nn.sigmoid(logits)

    totals = []
    for s, order in enumerate(orders):
        total = half(held[s], me // order[0] % 2) + arrived[s].astype(F32)
        for bit in order[1:-1]:
            mine = me // bit % 2
            part = swap(half(total, 1 - mine).astype(BF16), bit, size)
            total = half(total, mine) + part.astype(F32)
        totals.append((total, total.astype(BF16)))
    up = [turn(rank_up, s * cut, cut, after) for s, after in enumerate((sent[1], totals[1][1]))]
    terms = []
    for s, order in enumerate(orders):
        total, message = totals[s]
        total = total + swap(message, order[-1], size).astype(F32)
        have = jnp.tanh(total).astype(BF16)
        for bit in order[:-1][::-1]:
            part = swap(have, bit, size)
            low = me // bit % 2 == 0
            have = jnp.concatenate([jnp.where(low, have, part), jnp.where(low, part, have)], axis=2)
        for e in range(experts):
            terms.append(
                gate[e][:, None]
                * jnp.dot(have[e], up[s][e], preferred_element_type=F32)
            )
    bias = sum(gate[e][:, None] * expert_bias[e][None] for e in range(experts))
    blended = sum(terms, bias)
    inputs = samples.astype(F32)
    return (inputs * blended + inputs).astype(BF16)


def solution(mesh):
    placed = (
        P("batch", "width"),
        P("width", None, None),
        P(None, None, "width"),
        P("width", None),
        P(None, "width"),
    )
    return jax.shard_map(
        layer, mesh=mesh, in_specs=placed, out_specs=P("batch", "width"), check_vma=False
    )
```
